32 devices in a mesh: shell: 2 (over x), pix: 16 (over z, y, core).
Axes of the slice: x: 2, y: 2, z: 4, core: 2. Of those that a mesh axis runs over, the one named last changes fastest.
Arguments:
- block_tile: int32 [4, 1024], P('shell'), may hold values from 0 to 2047, as said below
- cell_index: int32 [4, 1024, 512], P('shell', 'pix'), may hold values from 0 to 2047
- masses: bfloat16 [4, 1024, 512], P('shell', 'pix'), may hold values from 0.125 to 8, as said below
- plane_coef: float32 [4], P('shell'), may hold values from 0.1 to 0.4
- plane_dist: float32 [4], P('shell'), may hold values from 0.2 to 1
- source_inv: float32 [4], P('shell'), may hold values from 0.5 to 1
Outputs:
- convergence: float32 [4, 2048, 2048], P('shell', 'pix')
- shear_one: float32 [4, 2048, 2048], P('shell', 'pix')
- shear_two: float32 [4, 2048, 2048], P('shell', 'pix')
The draws below stay inside these ranges and needn't reach their ends.
Inputs may be any that keep to these rules, and one draw needn't show every extreme that they name: `block_tile`: each row is 16 aligned runs of 64 entries, one run per index of pix. The entries of a run are distinct, and at most 8 of them lie in one index's rows of tiles (tile b lies in the rows of index b // 128). In every plane some index receives exactly 8 tiles from every run. `masses`: positive particle weights.
All inputs are finite; a program needn't handle non-finite values.
Results may differ from the reference program's by a relative error of at most 0.0003.
Values sent between devices are 32-bit elements; how exact they have to be, the bound alone decides.
A program may use at most 64 MiB of HBM per device.

```python
import math
import jax
import jax.numpy as jnp
from jax import lax

L = 2048
TR = 16
TC = 128
LT = 64
BPT = 4
PLANES = 4
TILES = 2048
TPO = 128
CAP = 8
N_PIX = 16


def draw_block_tile(key, part):
    owners = TILES // TPO
    slot_count = owners * CAP
    key_full = jax.random.fold_in(key, 11)
    key_order = jax.random.fold_in(key, 12)
    key_base = jax.random.fold_in(key, 13)
    full_owner = jax.random.randint(key_full, (PLANES, 1, 1), 0, owners)
    slot_ids = jnp.arange(slot_count)
    scores = jax.random.randint(key_order, (PLANES, owners, slot_count), 0, 1 << 20) * slot_count + slot_ids
    scores = jnp.where((slot_ids // CAP)[None, None, :] == full_owner, scores - (1 << 30), scores)
    chosen = jnp.argsort(scores, axis=-1)[:, :, :LT]
    owner_id = chosen // CAP
    rank_id = chosen % CAP
    base = jax.random.randint(key_base, (PLANES, owners, owners), 0, TPO)
    offset = jnp.take_along_axis(base, owner_id, axis=-1)
    tile_id = owner_id * TPO + (offset + rank_id) % TPO
    return tile_id.reshape(PLANES, owners * LT).astype(jnp.int32)


def draw_masses(key, part):
    owners = TILES // TPO
    scale_key = jax.random.fold_in(key, 21)
    single_key = jax.random.fold_in(key, 22)
    device_scale = jnp.exp(jax.random.uniform(scale_key, (PLANES, owners, 1, 1), jnp.float32, math.log(0.25), math.log(4.0)))
    particle = jnp.exp(jax.random.uniform(single_key, (PLANES, owners, LT, BPT * 128), jnp.float32, math.log(0.5), math.log(2.0)))
    return (device_scale * particle).reshape(PLANES, owners * LT, BPT * 128).astype(jnp.bfloat16)


def place_ends(result, own_key, low, high):
    extent = result.shape
    index_at = [jax.random.randint(jax.random.fold_in(own_key, axis), (), 0, extent[axis]) for axis in range(len(extent))]
    result = result.at[tuple(index_at)].set(low)
    longest = extent.index(max(extent))
    index_at[longest] = (index_at[longest] + 1) % extent[longest]
    return result.at[tuple(index_at)].set(high)


def levels(key, shape, split, least, top_value):
    factor_of = 1.0
    for axis_at, parts in split:
        heights = jax.random.uniform(jax.random.fold_in(jax.random.fold_in(key, 6), axis_at), (parts,), jnp.float32, least / len(split), top_value / len(split))
        factor_of = factor_of * jnp.repeat(jnp.exp(heights), shape[axis_at] // parts).reshape((-1,) + (1,) * (len(shape) - 1 - axis_at))
    return factor_of


def setup_inputs(seed: int = 0) -> dict:
    splits = jax.random.split(jax.random.key(seed), 7)
    return {
        "block_tile": draw_block_tile(jax.random.fold_in(splits[6], 71), 0),
        "cell_index": place_ends(jax.random.randint(splits[1], (PLANES, N_PIX * LT, BPT * 128), 0, TR * TC), jax.random.fold_in(splits[1], 1), 0, (TR * TC) - 1).astype(jnp.int32),
        "masses": draw_masses(jax.random.fold_in(splits[6], 71), 0),
        "plane_coef": jnp.clip(jnp.exp(math.log(0.4) - 1.3862944 * jax.random.uniform(splits[3], (PLANES,), jnp.float32) ** levels(splits[3], (PLANES,), ((0, 2),), -0.2, 0.2)), 0.1, 0.4),
        "plane_dist": jnp.clip(jnp.exp(math.log(1.0) - 1.609438 * jax.random.uniform(splits[4], (PLANES,), jnp.float32) ** levels(splits[4], (PLANES,), ((0, 2),), -0.2, 0.2)), 0.2, 1.0),
        "source_inv": jnp.clip(jnp.exp(math.log(1.0) - 0.6931472 * jax.random.uniform(splits[5], (PLANES,), jnp.float32) ** levels(splits[5], (PLANES,), ((0, 2),), -0.2, 0.2)), 0.5, 1.0),
    }


def reference(block_tile, cell_index, masses, plane_coef, plane_dist, source_inv):
    tiles_wide = L // TC

    def deposit(item):
        tile_ids, cell_ids, weights = item
        tile_col = tile_ids[:, None]
        pixel_row = (tile_col // tiles_wide) * TR + cell_ids // TC
        pixel_col = (tile_col % tiles_wide) * TC + cell_ids % TC
        flat_index = (pixel_row * L + pixel_col).reshape(-1).astype(jnp.int32)
        plane_sum = jnp.zeros((L * L,), jnp.float32).at[flat_index].add(weights.reshape(-1).astype(jnp.float32))
        plane_sum = plane_sum.reshape(L, L)
        mean_mass = jnp.sum(plane_sum) / (L * L)
        return plane_sum / mean_mass - 1.0

    contrast = lax.map(deposit, (block_tile, cell_index, masses))
    near_sum = jnp.cumsum(plane_coef[:, None, None] * contrast, axis=0)
    far_sum = jnp.cumsum((plane_coef * plane_dist)[:, None, None] * contrast, axis=0)
    convergence = near_sum - source_inv[:, None, None] * far_sum

    frequency = jnp.arange(L)
    signed = jnp.where(frequency >= L // 2, frequency - L, frequency).astype(jnp.float32)
    keep_mask = (frequency != L // 2).astype(jnp.float32)
    wave_x = signed[None, :]
    wave_y = signed[:, None]
    wave_power = jnp.maximum(wave_x * wave_x + wave_y * wave_y, 1.0)
    both_keep = keep_mask[None, :] * keep_mask[:, None]
    kernel_one = both_keep * (wave_x * wave_x - wave_y * wave_y) / wave_power
    kernel_two = both_keep * 2.0 * wave_x * wave_y / wave_power

    def shear(field):
        spectrum = jnp.fft.fft2(field)
        first = jnp.real(jnp.fft.ifft2(spectrum * kernel_one)).astype(jnp.float32)
        second = jnp.real(jnp.fft.ifft2(spectrum * kernel_two)).astype(jnp.float32)
        return first, second

    shear_one, shear_two = lax.map(shear, convergence)
    return convergence, shear_one, shear_two
```

```python
from functools import partial
import math

import jax
import jax.numpy as jnp
from jax import lax
from jax.experimental import pallas as pl
from jax.experimental.pallas import tpu as pltpu
from jax.sharding import PartitionSpec as P
import numpy as np

L = 2048
TR = 16
TC = 128


HIGHEST = lax.Precision.HIGHEST


def entering(value, axis, join, neutral):
    count, mine = (lax.axis_size(axis), lax.axis_index(axis))
    pieces = jax.tree.map(lambda part: lax.all_gather(part, axis), value)
    running = jax.tree.map(
        lambda part, zero: jnp.full_like(part, 0) + jnp.asarray(zero, part.dtype), value, neutral
    )

    def lap(position, running):
        longer = join(running, jax.tree.map(lambda part: part[position], pieces))
        return jax.tree.map(lambda new, old: jnp.where(position < mine, new, old), longer, running)

    return lax.fori_loop(0, count - 1, lap, running)


def dft_table(left_size, right_size, period, sign_value):
    left_idx = jnp.arange(left_size)[:, None]
    right_idx = jnp.arange(right_size)[None, :]
    angle = 2.0 * math.pi / period * (left_idx * right_idx % period).astype(jnp.float32)
    return (jnp.cos(angle), sign_value * jnp.sin(angle))


def mix_outer(table, real_part, imag_part):
    cosine, sine_part = table
    contract = partial(jnp.einsum, "ab,...bc->...ac", precision=HIGHEST)
    return (
        contract(cosine, real_part) - contract(sine_part, imag_part),
        contract(sine_part, real_part) + contract(cosine, imag_part),
    )


def mix_inner(table, real_part, imag_part):
    cosine, sine_part = table
    product = partial(jnp.matmul, precision=HIGHEST)
    return (
        product(real_part, cosine) - product(imag_part, sine_part),
        product(real_part, sine_part) + product(imag_part, cosine),
    )


def twist(table, real_part, imag_part):
    cosine, sine_part = table
    return (real_part * cosine - imag_part * sine_part, real_part * sine_part + imag_part * cosine)


def transform_last(real_part, imag_part, sign_value):
    length = real_part.shape[-1]
    inner = math.gcd(length, 128)
    outer = length // inner
    leading = real_part.shape[:-1]
    real_part = real_part.reshape(leading + (outer, inner))
    imag_part = imag_part.reshape(leading + (outer, inner))
    outer_table = dft_table(outer, outer, outer, sign_value)
    inner_table = dft_table(inner, inner, inner, sign_value)
    twiddle = dft_table(outer, inner, length, sign_value)
    if sign_value < 0:
        real_part, imag_part = mix_outer(outer_table, real_part, imag_part)
        real_part, imag_part = twist(twiddle, real_part, imag_part)
        real_part, imag_part = mix_inner(inner_table, real_part, imag_part)
    else:
        real_part, imag_part = mix_inner(inner_table, real_part, imag_part)
        real_part, imag_part = twist(twiddle, real_part, imag_part)
        real_part, imag_part = mix_outer(outer_table, real_part, imag_part)
    return (real_part.reshape(leading + (length,)), imag_part.reshape(leading + (length,)))


def frequency_of(position, length):
    inner = math.gcd(length, 128)
    outer = length // inner
    frequency = position // inner + outer * (position % inner)
    signed = jnp.where(frequency >= length // 2, frequency - length, frequency).astype(jnp.float32)
    keep_mask = (frequency != length // 2).astype(jnp.float32)
    return (signed, keep_mask)


def add_pairs(earlier_pair, later_pair):
    return (earlier_pair[0] + later_pair[0], earlier_pair[1] + later_pair[1])


def deposit_group(item):
    cell_ids, weights = item
    tile_rows = cell_ids // TC
    tile_cols = cell_ids % TC
    row_hot = jnp.where(
        tile_rows[:, None, :] == jnp.arange(TR)[None, :, None],
        weights[:, None, :],
        jnp.zeros((), jnp.bfloat16),
    )
    col_hot = (tile_cols[:, :, None] == jnp.arange(TC)[None, None, :]).astype(jnp.bfloat16)
    return jnp.einsum("grk,gkc->grc", row_hot, col_hot, preferred_element_type=jnp.float32)


def rows_to_sending(packed, groups, slab, cols_own):
    count, fields = (packed.shape[0], packed.shape[1])
    return (
        packed.reshape(count, fields, slab, groups, cols_own)
        .transpose(3, 0, 1, 4, 2)
        .reshape(groups, count, fields, cols_own * slab)
    )


def arrived_to_columns(arrived, groups, slab, cols_own):
    count, fields = (arrived.shape[1], arrived.shape[2])
    return (
        arrived.reshape(groups, count, fields, cols_own, slab)
        .transpose(1, 2, 3, 0, 4)
        .reshape(count, fields, cols_own, groups * slab)
    )


def columns_to_sending(stacked, groups, slab, cols_own):
    count, fields = (stacked.shape[0], stacked.shape[1])
    return (
        stacked.reshape(count, fields, cols_own, groups, slab)
        .transpose(3, 0, 1, 2, 4)
        .reshape(groups, count, fields, cols_own * slab)
    )


def landed_to_rows(landed, groups, slab, cols_own):
    count, fields = (landed.shape[1], landed.shape[2])
    return (
        landed.reshape(groups, count, fields, cols_own, slab)
        .transpose(1, 2, 4, 0, 3)
        .reshape(count, fields, slab, groups * cols_own)
    )


def local(block_tile, cell_index, masses, plane_coef, plane_dist, source_inv):
    groups = lax.axis_size("pix")
    my_index = lax.axis_index("pix")
    planes, local_tiles, per_tile = cell_index.shape
    slab = L // groups
    per_owner = slab // TR * (L // TC)
    cap = max(1, 2 * local_tiles // groups)
    flat = TR * TC
    batch_tiles = 8
    deposited = lax.map(
        deposit_group,
        (cell_index.reshape(-1, batch_tiles, per_tile), masses.reshape(-1, batch_tiles, per_tile)),
    )
    tile_sums = deposited.reshape(planes, local_tiles, flat)
    table = block_tile.reshape(planes, groups, local_tiles)
    owner = table // per_owner
    earlier = jnp.arange(local_tiles)[:, None] < jnp.arange(local_tiles)[None, :]
    same_owner = owner[:, :, :, None] == owner[:, :, None, :]
    rank = jnp.sum(jnp.where(same_owner & earlier[None, None], 1, 0), axis=2)
    slot = owner * cap + rank
    my_slots = lax.dynamic_index_in_dim(slot, my_index, axis=1, keepdims=False)
    slot_grid = jnp.arange(groups)[:, None] * cap + jnp.arange(cap)[None, :]
    send_hot = (my_slots[:, None, None, :] == slot_grid[None, :, :, None]).astype(jnp.float32)
    outgoing = jnp.einsum("pnct,ptf->npcf", send_hot, tile_sums, precision=HIGHEST)
    incoming = lax.all_to_all(outgoing, "pix", split_axis=0, concat_axis=0, tiled=True)
    local_index = table - my_index * per_owner
    is_mine = owner == my_index
    tile_hot = (is_mine[..., None] & (local_index[..., None] == jnp.arange(per_owner))).astype(
        jnp.float32
    )
    slot_hot = (rank[..., None] == jnp.arange(cap)).astype(jnp.float32)
    placing = jnp.einsum("pstl,pstc->plsc", tile_hot, slot_hot, precision=HIGHEST)
    slab_tiles = jnp.einsum("plsc,spcf->plf", placing, incoming, precision=HIGHEST)
    density = (
        slab_tiles.reshape(planes, slab // TR, L // TC, TR, TC)
        .transpose(0, 1, 3, 2, 4)
        .reshape(planes, slab, L)
    )
    total = lax.psum(jnp.sum(density, axis=(1, 2)), "pix")
    contrast = density / (total / (L * L))[:, None, None] - 1.0
    near_local = jnp.cumsum(plane_coef[:, None, None] * contrast, axis=0)
    far_local = jnp.cumsum((plane_coef * plane_dist)[:, None, None] * contrast, axis=0)
    blank = jnp.zeros((slab, L), jnp.float32)
    near_before, far_before = entering(
        (near_local[-1], far_local[-1]), "shell", add_pairs, (blank, blank)
    )
    convergence = near_before + near_local - source_inv[:, None, None] * (far_before + far_local)
    cols_own = L // groups
    wave_x, keep_x = frequency_of(my_index * cols_own + jnp.arange(cols_own), L)
    wave_y, keep_y = frequency_of(jnp.arange(L), L)
    wave_x = wave_x[:, None]
    wave_y = wave_y[None, :]
    both_keep = keep_x[:, None] * keep_y[None, :]
    wave_power = jnp.maximum(wave_x * wave_x + wave_y * wave_y, 1.0)
    kernel_one = both_keep * (wave_x * wave_x - wave_y * wave_y) / wave_power
    kernel_two = both_keep * 2.0 * wave_x * wave_y / wave_power
    scale = 1.0 / (L * L)
    spec_real, spec_imag = transform_last(convergence[0::2], convergence[1::2], -1.0)
    sending = rows_to_sending(jnp.stack([spec_real, spec_imag], axis=1), groups, slab, cols_own)
    arrived = lax.all_to_all(sending, "pix", split_axis=0, concat_axis=0, tiled=True)
    columns = arrived_to_columns(arrived, groups, slab, cols_own)
    row_real, row_imag = transform_last(columns[:, 0], columns[:, 1], -1.0)
    first_real, first_imag = transform_last(row_real * kernel_one, row_imag * kernel_one, 1.0)
    second_real, second_imag = transform_last(row_real * kernel_two, row_imag * kernel_two, 1.0)
    stacked = jnp.stack([first_real, first_imag, second_real, second_imag], axis=1)
    landed = lax.all_to_all(
        columns_to_sending(stacked, groups, slab, cols_own),
        "pix",
        split_axis=0,
        concat_axis=0,
        tiled=True,
    )
    row_layout = landed_to_rows(landed, groups, slab, cols_own)
    even_one, odd_one = transform_last(row_layout[:, 0], row_layout[:, 1], 1.0)
    even_two, odd_two = transform_last(row_layout[:, 2], row_layout[:, 3], 1.0)
    shear_one = jnp.stack([even_one, odd_one], axis=1).reshape(planes, slab, L)
    shear_two = jnp.stack([even_two, odd_two], axis=1).reshape(planes, slab, L)
    return (convergence, shear_one * scale, shear_two * scale)


INNER = 128
OUTER = L // INNER
HALF_BLOCKS = OUTER // 2


def block_columns():
    cols = np.zeros((HALF_BLOCKS, INNER), np.int64)
    for b in range(HALF_BLOCKS - 1):
        cols[b] = b + 1 + OUTER * np.arange(INNER)
    half = np.arange(INNER // 2)
    cols[-1] = np.concatenate([OUTER * half, HALF_BLOCKS + OUTER * half])
    return cols


def split_table(table):
    high = table.astype(jnp.bfloat16)
    low = (table - high.astype(np.float64)).astype(jnp.bfloat16)
    return high, low


def row_tables():
    n2 = np.arange(INNER)
    out = np.zeros((HALF_BLOCKS, 2 * INNER, 2 * INNER))
    cols = block_columns()
    for b in range(HALF_BLOCKS):
        angle = 2 * np.pi / L * ((n2[:, None] * cols[b][None, :]) % L)
        co, si = np.cos(angle), np.sin(angle)
        if b < HALF_BLOCKS - 1:
            out[b] = np.block([[co, -si], [si, co]])
        else:
            h = INNER // 2
            out[b, :INNER, :h] = co[:, :h]
            out[b, :INNER, INNER : INNER + h] = -si[:, :h]
            out[b, INNER:, h:INNER] = co[:, h:]
            out[b, INNER:, INNER + h :] = -si[:, h:]
    return split_table(out)


def column_tables():
    idx = np.arange(INNER)
    angle = 2 * np.pi / INNER * ((idx[:, None] * idx[None, :]) % INNER)
    co, si = np.cos(angle), np.sin(angle)
    return split_table(np.block([[co, si], [-si, co]]))


def twiddle_tables():
    angle = 2 * np.pi / L * (np.arange(OUTER)[:, None] * np.arange(INNER)[None, :])
    return np.cos(angle).astype(np.float32), (-np.sin(angle)).astype(np.float32)


def times_root(value, k, n, sign):
    re, im = value
    k = k % n
    if k == 0:
        return value
    if 4 * k == n:
        return (-im, re) if sign > 0 else (im, -re)
    angle = 2 * math.pi * k / n
    c, s = math.cos(angle), sign * math.sin(angle)
    if 8 * k == n or 8 * k == 3 * n:
        if c > 0:
            return ((re - im) * c, (re + im) * c) if sign > 0 else ((re + im) * c, (im - re) * c)
        c = -c
        return ((re + im) * -c, (re - im) * c) if sign > 0 else ((im - re) * c, (re + im) * -c)
    return (re * c - im * s, re * s + im * c)


def fft_list(values, sign):
    n = len(values)
    if n == 1:
        return values
    even = fft_list(values[0::2], sign)
    odd = fft_list(values[1::2], sign)
    odd = [times_root(v, k, n, sign) for k, v in enumerate(odd)]
    return [(a[0] + b[0], a[1] + b[1]) for a, b in zip(even, odd)] + [
        (a[0] - b[0], a[1] - b[1]) for a, b in zip(even, odd)
    ]


def split_value(value):
    high = value.astype(jnp.bfloat16)
    return high, (value - high.astype(jnp.float32)).astype(jnp.bfloat16)


def three_pass(left, right, dims):
    dot = lambda a, b: lax.dot_general(a, b, (dims, ((), ())), preferred_element_type=jnp.float32)
    return dot(left[0], right[0]) + (dot(left[0], right[1]) + dot(left[1], right[0]))


def deposit_kernel(slot_ref, cell_ref, mass_ref, *out_refs):
    planes, tiles, per_tile = cell_ref.shape
    groups, rows, _ = out_refs[0].shape
    cap = rows // TR
    row_id = lax.broadcasted_iota(jnp.int32, (TR, per_tile), 0)
    col_id = lax.broadcasted_iota(jnp.int32, (TC, per_tile), 0)
    for p in range(planes):
        out_ref = out_refs[p]
        out_ref[...] = jnp.zeros_like(out_ref)
        total = jnp.sum(jnp.sum(mass_ref[p].astype(jnp.float32), axis=0, keepdims=True), axis=1, keepdims=True)
        out_ref[:, cap * TR :, :] = jnp.broadcast_to(total[None], (groups, rows - cap * TR, TC))

        def batch(g, _):
            base = pl.multiple_of(g * 16, 16)
            cells = cell_ref[p, pl.ds(base, 16), :]
            weights = mass_ref[p, pl.ds(base, 16), :].astype(jnp.float32)
            for i in range(16):
                cell = cells[i : i + 1]
                weight = weights[i : i + 1]
                row_hot = jnp.where(row_id == cell // TC, weight, 0.0).astype(jnp.bfloat16)
                col_hot = jnp.where(col_id == cell % TC, 1.0, 0.0).astype(jnp.bfloat16)
                tile = lax.dot_general(
                    row_hot, col_hot, (((1,), (1,)), ((), ())), preferred_element_type=jnp.float32
                )
                slot = slot_ref[p, base + i]
                out_ref[slot // cap, pl.ds(pl.multiple_of((slot % cap) * TR, TR), TR), :] = tile
            return 0

        lax.fori_loop(0, tiles // 16, batch, 0)


def assemble_kernel(place_ref, in_ref, out_ref, held):
    groups, rows, _ = in_ref.shape
    cap = rows // TR
    tiles = out_ref.shape[0]
    held[...] = jnp.zeros_like(held)
    total = in_ref[0, cap * TR : cap * TR + 1, 0:1]
    for s in range(1, groups):
        total = total + in_ref[s, cap * TR : cap * TR + 1, 0:1]

    def source(s, _):
        for c in range(cap):
            at = place_ref[s * cap + c]
            held[at] = held[at] + in_ref[s, c * TR : (c + 1) * TR, :]
        return 0

    lax.fori_loop(0, groups, source, 0)
    factor = (L * L) / total
    out_ref[...] = held[0:tiles] * factor[None] - 1.0


def row_forward_kernel(mix_ref, near0, near1, far0, far1, high_ref, low_ref, conv_ref, out_ref, held):
    tile_rows = near0.shape[0] // OUTER

    def chunk(t, _):
        rows = pl.ds(pl.multiple_of(t * TR, TR), TR)
        packed = []
        for n in range(OUTER):
            at = t * OUTER + n
            fields = (near0[at], near1[at], far0[at], far1[at])
            pair = []
            for i in range(2):
                value = mix_ref[i, 0] * fields[0]
                for j in range(1, 4):
                    value = value + mix_ref[i, j] * fields[j]
                conv_ref[i, rows, n * INNER : (n + 1) * INNER] = value
                pair.append(value)
            packed.append(tuple(pair))
        z = fft_list(packed, -1)
        for k in range(1, HALF_BLOCKS):
            (ar, ai), (br, bi) = z[k], z[OUTER - k]
            held[k - 1, 0, rows, :INNER] = 0.5 * (ar + br)
            held[k - 1, 0, rows, INNER:] = 0.5 * (ai - bi)
            held[k - 1, 1, rows, :INNER] = 0.5 * (ai + bi)
            held[k - 1, 1, rows, INNER:] = 0.5 * (br - ar)
        for p in range(2):
            held[HALF_BLOCKS - 1, p, rows, :INNER] = z[0][p]
            held[HALF_BLOCKS - 1, p, rows, INNER:] = z[HALF_BLOCKS][p]
        return 0

    lax.fori_loop(0, tile_rows, chunk, 0)

    def block(b, _):
        slab = tile_rows * TR
        value = held[b].reshape(2 * slab, 2 * INNER)
        result = three_pass(split_value(value), (high_ref[b], low_ref[b]), ((1,), (0,)))
        for p in range(2):
            for half in range(2):
                out_ref[b, p, half] = result[
                    p * slab : (p + 1) * slab, half * INNER : (half + 1) * INNER
                ]
        return 0

    lax.fori_loop(0, HALF_BLOCKS, block, 0)


def column_kernel(in_ref, col_ref, twr_ref, twi_ref, high_ref, low_ref, back_high_ref, back_low_ref, out_ref, held, *back):
    def twist_of(k, rows):
        return twr_ref[k, rows, :], twi_ref[k, rows, :]

    def forward(t, _):
        rows = pl.ds(pl.multiple_of(t * 8, 8), 8)
        z = fft_list([(in_ref[n, 0, rows, :], in_ref[n, 1, rows, :]) for n in range(OUTER)], -1)
        for k in range(OUTER):
            re, im = z[k]
            if k:
                c, s = twist_of(k, rows)
                re, im = re * c - im * s, re * s + im * c
            held[k, 0, rows, :] = re
            held[k, 1, rows, :] = im
        return 0

    lax.fori_loop(0, INNER // 8, forward, 0)
    signed_v = col_ref[0:1]
    weight = col_ref[1:2]
    inner_id = lax.broadcasted_iota(jnp.int32, (INNER, INNER), 0)

    def middle(k, _):
        value = held[k].reshape(2 * INNER, INNER)
        spectrum = three_pass((high_ref[...], low_ref[...]), split_value(value), ((1,), (0,)))
        u = k + OUTER * inner_id
        signed_u = jnp.where(u >= L // 2, u - L, u).astype(jnp.float32)
        scale = jnp.where(u == L // 2, 0.0, weight)
        uu, vv = signed_u * signed_u, signed_v * signed_v
        over = scale / jnp.maximum(uu + vv, 1.0)
        kernels = ((vv - uu) * over, 2.0 * signed_v * signed_u * over)
        for f in range(2):
            twice = jnp.concatenate([kernels[f], kernels[f]], axis=0)
            result = three_pass(
                (back_high_ref[...], back_low_ref[...]), split_value(spectrum * twice), ((1,), (0,))
            )
            re, im = result[:INNER], result[INNER:]
            c, s = twr_ref[k], twi_ref[k]
            back[f][k, 0] = re * c + im * s
            back[f][k, 1] = im * c - re * s
        return 0

    lax.fori_loop(0, OUTER, middle, 0)
    for f in range(2):

        def inverse(t, _):
            rows = pl.ds(pl.multiple_of(t * 8, 8), 8)
            x = fft_list([(back[f][k, 0, rows, :], back[f][k, 1, rows, :]) for k in range(OUTER)], 1)
            for n in range(OUTER):
                out_ref[n, f, 0, rows, :] = x[n][0]
                out_ref[n, f, 1, rows, :] = x[n][1]
            return 0

        lax.fori_loop(0, INNER // 8, inverse, 0)


def row_inverse_kernel(in_ref, high_ref, low_ref, one_ref, two_ref, held):
    slab = in_ref.shape[4]
    for f, out_ref in enumerate((one_ref, two_ref)):

        def block(b, _):
            value = jnp.concatenate(
                [jnp.concatenate([in_ref[b, p, f, 0], in_ref[b, p, f, 1]], axis=1) for p in range(2)], axis=0
            )
            held[b] = three_pass(split_value(value), (high_ref[b], low_ref[b]), ((1,), (1,))).reshape(
                2, slab, 2 * INNER
            )
            return 0

        lax.fori_loop(0, HALF_BLOCKS, block, 0)

        def chunk(t, _):
            rows = pl.ds(pl.multiple_of(t * 8, 8), 8)
            z = [None] * OUTER
            last = HALF_BLOCKS - 1
            z[0] = (held[last, 0, rows, :INNER], held[last, 1, rows, :INNER])
            z[HALF_BLOCKS] = (held[last, 0, rows, INNER:], held[last, 1, rows, INNER:])
            for k in range(1, HALF_BLOCKS):
                ar, ai = held[k - 1, 0, rows, :INNER], held[k - 1, 0, rows, INNER:]
                br, bi = held[k - 1, 1, rows, :INNER], held[k - 1, 1, rows, INNER:]
                z[k] = (ar - bi, ai + br)
                z[OUTER - k] = (ar + bi, br - ai)
            x = fft_list(z, 1)
            for n in range(OUTER):
                for p in range(2):
                    out_ref[p, rows, n * INNER : (n + 1) * INNER] = x[n][p]
            return 0

        lax.fori_loop(0, slab // 8, chunk, 0)


def call(body, outs, scratch=(), smem=(0,), count=1, megabytes=48, flops=0):
    space = [
        pl.BlockSpec(memory_space=pltpu.SMEM if i in smem else pltpu.VMEM) for i in range(count)
    ]
    return pl.pallas_call(
        body,
        out_shape=outs,
        in_specs=space,
        out_specs=jax.tree.map(lambda _: pl.BlockSpec(memory_space=pltpu.VMEM), outs),
        scratch_shapes=list(scratch),
        compiler_params=pltpu.CompilerParams(vmem_limit_bytes=megabytes << 20),
        cost_estimate=pl.CostEstimate(flops=flops, bytes_accessed=4 << 20, transcendentals=0),
    )


def shape(*dims):
    return jax.ShapeDtypeStruct(dims, jnp.float32)


def local_fast(block_tile, cell_index, masses, plane_coef, plane_dist, source_inv):
    groups = lax.axis_size("pix")
    me = lax.axis_index("pix")
    mine_shell = lax.axis_index("shell")
    planes, local_tiles, per_tile = cell_index.shape
    slab = L // groups
    per_owner = slab // TR * (L // TC)
    cap = max(1, 2 * local_tiles // groups)

    pairs = [(0, 1)]
    other = lax.ppermute(jnp.concatenate([plane_coef, plane_dist]), "shell", pairs)
    other_coef = jnp.where(mine_shell > 0, other[:planes], 0.0)
    other_dist = other[planes:]

    table = block_tile.reshape(planes, groups, local_tiles)
    owner = table // per_owner
    earlier = jnp.arange(local_tiles)[:, None] < jnp.arange(local_tiles)[None, :]
    same_owner = owner[:, :, :, None] == owner[:, :, None, :]
    rank = jnp.sum(jnp.where(same_owner & earlier[None, None], 1, 0), axis=2)
    slot = owner * cap + rank
    my_slots = lax.dynamic_index_in_dim(slot, me, axis=1, keepdims=False)
    wanted = me * cap + jnp.arange(cap)
    here = slot[:, :, None, :] == wanted[None, None, :, None]
    local_index = table - me * per_owner
    place = jnp.sum(jnp.where(here, local_index[:, :, None, :] + 1, 0), axis=3)
    place = jnp.where(place > 0, place - 1, per_owner).reshape(planes, groups * cap)

    rows = cap * TR + 8
    outgoing = call(deposit_kernel, [shape(groups, rows, TC)] * planes, count=3, flops=1 << 29)(
        my_slots, cell_index, masses
    )
    near, far = [], []
    for p in range(planes):
        incoming = lax.all_to_all(outgoing[p], "pix", split_axis=0, concat_axis=0, tiled=True)
        contrast = call(
            assemble_kernel,
            shape(per_owner, TR, TC),
            [pltpu.VMEM((per_owner + 1, TR, TC), jnp.float32)],
            count=2,
            flops=1 << 22,
        )(place[p], incoming)
        near.append(contrast)
        far.append(lax.ppermute(contrast, "shell", pairs))

    own = plane_coef[None, :] * (1.0 - source_inv[:, None] * plane_dist[None, :])
    own = jnp.where(jnp.arange(planes)[None, :] <= jnp.arange(planes)[:, None], own, 0.0)
    before = other_coef[None, :] * (1.0 - source_inv[:, None] * other_dist[None, :])
    mix = jnp.concatenate([own, before], axis=1)

    row_high, row_low = row_tables()
    convergence, sending = call(
        row_forward_kernel,
        [shape(planes, slab, L), shape(HALF_BLOCKS, planes, 2, slab, INNER)],
        [pltpu.VMEM((HALF_BLOCKS, planes, slab, 2 * INNER), jnp.float32)],
        count=7,
        flops=1 << 30,
    )(mix, *near, *far, row_high, row_low)
    arrived = lax.all_to_all(
        sending.reshape(groups, 2, slab, INNER), "pix", split_axis=0, concat_axis=0, tiled=True
    )

    columns = jnp.asarray(block_columns().astype(np.float32))
    mine = lax.dynamic_index_in_dim(columns, me // planes, axis=0, keepdims=False)
    special = (me // planes == HALF_BLOCKS - 1) & (mine > 0)
    weight = jnp.where(special, 2.0, 1.0) / (L * L)
    signed = jnp.where(mine >= L // 2, mine - L, mine)
    col_info = jnp.stack([signed, weight])
    col_high, col_low = column_tables()
    tw_real, tw_imag = twiddle_tables()
    spread = lambda t: jnp.broadcast_to(jnp.asarray(t)[:, :, None], (OUTER, INNER, INNER))
    leaving = call(
        column_kernel,
        shape(groups, 2, 2, slab, INNER),
        [pltpu.VMEM((OUTER, 2, INNER, INNER), jnp.float32)] * 3,
        smem=(),
        count=8,
        flops=1 << 31,
    )(arrived, col_info, spread(tw_real), spread(tw_imag), col_high, col_low, col_high.T.copy(), col_low.T.copy())
    landed = lax.all_to_all(leaving, "pix", split_axis=0, concat_axis=0, tiled=True)
    shear_one, shear_two = call(
        row_inverse_kernel,
        [shape(planes, slab, L)] * 2,
        [pltpu.VMEM((HALF_BLOCKS, planes, slab, 2 * INNER), jnp.float32)],
        smem=(),
        count=3,
        flops=1 << 31,
    )(landed.reshape(HALF_BLOCKS, planes, 2, 2, slab, INNER), row_high, row_low)
    return convergence, shear_one, shear_two


def solution(mesh):
    placed = (
        P("shell", None),
        P("shell", "pix", None),
        P("shell", "pix", None),
        P("shell"),
        P("shell"),
        P("shell"),
    )
    shells, groups = mesh.shape["shell"], mesh.shape["pix"]

    def body(block_tile, cell_index, *rest):
        fits = (
            shells == 2
            and cell_index.shape[0] == 2
            and groups == OUTER
            and cell_index.shape[1] % 16 == 0
        )
        return (local_fast if fits else local)(block_tile, cell_index, *rest)

    return jax.shard_map(
        body,
        mesh=mesh,
        in_specs=placed,
        out_specs=(P("shell", "pix", None), P("shell", "pix", None), P("shell", "pix", None)),
        check_vma=False,
    )
```

```python
from functools import partial
import math

import jax
import jax.numpy as jnp
from jax import lax
from jax.experimental import pallas as pl
from jax.experimental.pallas import tpu as pltpu
from jax.sharding import PartitionSpec as P
import numpy as np

L = 2048
TR = 16
TC = 128


HIGHEST = lax.Precision.HIGHEST


def entering(value, axis, join, neutral):
    count, mine = (lax.axis_size(axis), lax.axis_index(axis))
    pieces = jax.tree.map(lambda part: lax.all_gather(part, axis), value)
    running = jax.tree.map(
        lambda part, zero: jnp.full_like(part, 0) + jnp.asarray(zero, part.dtype), value, neutral
    )

    def lap(position, running):
        longer = join(running, jax.tree.map(lambda part: part[position], pieces))
        return jax.tree.map(lambda new, old: jnp.where(position < mine, new, old), longer, running)

    return lax.fori_loop(0, count - 1, lap, running)


def dft_table(left_size, right_size, period, sign_value):
    left_idx = jnp.arange(left_size)[:, None]
    right_idx = jnp.arange(right_size)[None, :]
    angle = 2.0 * math.pi / period * (left_idx * right_idx % period).astype(jnp.float32)
    return (jnp.cos(angle), sign_value * jnp.sin(angle))


def mix_outer(table, real_part, imag_part):
    cosine, sine_part = table
    contract = partial(jnp.einsum, "ab,...bc->...ac", precision=HIGHEST)
    return (
        contract(cosine, real_part) - contract(sine_part, imag_part),
        contract(sine_part, real_part) + contract(cosine, imag_part),
    )


def mix_inner(table, real_part, imag_part):
    cosine, sine_part = table
    product = partial(jnp.matmul, precision=HIGHEST)
    return (
        product(real_part, cosine) - product(imag_part, sine_part),
        product(real_part, sine_part) + product(imag_part, cosine),
    )


def twist(table, real_part, imag_part):
    cosine, sine_part = table
    return (real_part * cosine - imag_part * sine_part, real_part * sine_part + imag_part * cosine)


def transform_last(real_part, imag_part, sign_value):
    length = real_part.shape[-1]
    inner = math.gcd(length, 128)
    outer = length // inner
    leading = real_part.shape[:-1]
    real_part = real_part.reshape(leading + (outer, inner))
    imag_part = imag_part.reshape(leading + (outer, inner))
    outer_table = dft_table(outer, outer, outer, sign_value)
    inner_table = dft_table(inner, inner, inner, sign_value)
    twiddle = dft_table(outer, inner, length, sign_value)
    if sign_value < 0:
        real_part, imag_part = mix_outer(outer_table, real_part, imag_part)
        real_part, imag_part = twist(twiddle, real_part, imag_part)
        real_part, imag_part = mix_inner(inner_table, real_part, imag_part)
    else:
        real_part, imag_part = mix_inner(inner_table, real_part, imag_part)
        real_part, imag_part = twist(twiddle, real_part, imag_part)
        real_part, imag_part = mix_outer(outer_table, real_part, imag_part)
    return (real_part.reshape(leading + (length,)), imag_part.reshape(leading + (length,)))


def frequency_of(position, length):
    inner = math.gcd(length, 128)
    outer = length // inner
    frequency = position // inner + outer * (position % inner)
    signed = jnp.where(frequency >= length // 2, frequency - length, frequency).astype(jnp.float32)
    keep_mask = (frequency != length // 2).astype(jnp.float32)
    return (signed, keep_mask)


def add_pairs(earlier_pair, later_pair):
    return (earlier_pair[0] + later_pair[0], earlier_pair[1] + later_pair[1])


def deposit_group(item):
    cell_ids, weights = item
    tile_rows = cell_ids // TC
    tile_cols = cell_ids % TC
    row_hot = jnp.where(
        tile_rows[:, None, :] == jnp.arange(TR)[None, :, None],
        weights[:, None, :],
        jnp.zeros((), jnp.bfloat16),
    )
    col_hot = (tile_cols[:, :, None] == jnp.arange(TC)[None, None, :]).astype(jnp.bfloat16)
    return jnp.einsum("grk,gkc->grc", row_hot, col_hot, preferred_element_type=jnp.float32)


def rows_to_sending(packed, groups, slab, cols_own):
    count, fields = (packed.shape[0], packed.shape[1])
    return (
        packed.reshape(count, fields, slab, groups, cols_own)
        .transpose(3, 0, 1, 4, 2)
        .reshape(groups, count, fields, cols_own * slab)
    )


def arrived_to_columns(arrived, groups, slab, cols_own):
    count, fields = (arrived.shape[1], arrived.shape[2])
    return (
        arrived.reshape(groups, count, fields, cols_own, slab)
        .transpose(1, 2, 3, 0, 4)
        .reshape(count, fields, cols_own, groups * slab)
    )


def columns_to_sending(stacked, groups, slab, cols_own):
    count, fields = (stacked.shape[0], stacked.shape[1])
    return (
        stacked.reshape(count, fields, cols_own, groups, slab)
        .transpose(3, 0, 1, 2, 4)
        .reshape(groups, count, fields, cols_own * slab)
    )


def landed_to_rows(landed, groups, slab, cols_own):
    count, fields = (landed.shape[1], landed.shape[2])
    return (
        landed.reshape(groups, count, fields, cols_own, slab)
        .transpose(1, 2, 4, 0, 3)
        .reshape(count, fields, slab, groups * cols_own)
    )


def local(block_tile, cell_index, masses, plane_coef, plane_dist, source_inv):
    groups = lax.axis_size("pix")
    my_index = lax.axis_index("pix")
    planes, local_tiles, per_tile = cell_index.shape
    slab = L // groups
    per_owner = slab // TR * (L // TC)
    cap = max(1, 2 * local_tiles // groups)
    flat = TR * TC
    batch_tiles = 8
    deposited = lax.map(
        deposit_group,
        (cell_index.reshape(-1, batch_tiles, per_tile), masses.reshape(-1, batch_tiles, per_tile)),
    )
    tile_sums = deposited.reshape(planes, local_tiles, flat)
    table = block_tile.reshape(planes, groups, local_tiles)
    owner = table // per_owner
    earlier = jnp.arange(local_tiles)[:, None] < jnp.arange(local_tiles)[None, :]
    same_owner = owner[:, :, :, None] == owner[:, :, None, :]
    rank = jnp.sum(jnp.where(same_owner & earlier[None, None], 1, 0), axis=2)
    slot = owner * cap + rank
    my_slots = lax.dynamic_index_in_dim(slot, my_index, axis=1, keepdims=False)
    slot_grid = jnp.arange(groups)[:, None] * cap + jnp.arange(cap)[None, :]
    send_hot = (my_slots[:, None, None, :] == slot_grid[None, :, :, None]).astype(jnp.float32)
    outgoing = jnp.einsum("pnct,ptf->npcf", send_hot, tile_sums, precision=HIGHEST)
    incoming = lax.all_to_all(outgoing, "pix", split_axis=0, concat_axis=0, tiled=True)
    local_index = table - my_index * per_owner
    is_mine = owner == my_index
    tile_hot = (is_mine[..., None] & (local_index[..., None] == jnp.arange(per_owner))).astype(
        jnp.float32
    )
    slot_hot = (rank[..., None] == jnp.arange(cap)).astype(jnp.float32)
    placing = jnp.einsum("pstl,pstc->plsc", tile_hot, slot_hot, precision=HIGHEST)
    slab_tiles = jnp.einsum("plsc,spcf->plf", placing, incoming, precision=HIGHEST)
    density = (
        slab_tiles.reshape(planes, slab // TR, L // TC, TR, TC)
        .transpose(0, 1, 3, 2, 4)
        .reshape(planes, slab, L)
    )
    total = lax.psum(jnp.sum(density, axis=(1, 2)), "pix")
    contrast = density / (total / (L * L))[:, None, None] - 1.0
    near_local = jnp.cumsum(plane_coef[:, None, None] * contrast, axis=0)
    far_local = jnp.cumsum((plane_coef * plane_dist)[:, None, None] * contrast, axis=0)
    blank = jnp.zeros((slab, L), jnp.float32)
    near_before, far_before = entering(
        (near_local[-1], far_local[-1]), "shell", add_pairs, (blank, blank)
    )
    convergence = near_before + near_local - source_inv[:, None, None] * (far_before + far_local)
    cols_own = L // groups
    wave_x, keep_x = frequency_of(my_index * cols_own + jnp.arange(cols_own), L)
    wave_y, keep_y = frequency_of(jnp.arange(L), L)
    wave_x = wave_x[:, None]
    wave_y = wave_y[None, :]
    both_keep = keep_x[:, None] * keep_y[None, :]
    wave_power = jnp.maximum(wave_x * wave_x + wave_y * wave_y, 1.0)
    kernel_one = both_keep * (wave_x * wave_x - wave_y * wave_y) / wave_power
    kernel_two = both_keep * 2.0 * wave_x * wave_y / wave_power
    scale = 1.0 / (L * L)
    spec_real, spec_imag = transform_last(convergence[0::2], convergence[1::2], -1.0)
    sending = rows_to_sending(jnp.stack([spec_real, spec_imag], axis=1), groups, slab, cols_own)
    arrived = lax.all_to_all(sending, "pix", split_axis=0, concat_axis=0, tiled=True)
    columns = arrived_to_columns(arrived, groups, slab, cols_own)
    row_real, row_imag = transform_last(columns[:, 0], columns[:, 1], -1.0)
    first_real, first_imag = transform_last(row_real * kernel_one, row_imag * kernel_one, 1.0)
    second_real, second_imag = transform_last(row_real * kernel_two, row_imag * kernel_two, 1.0)
    stacked = jnp.stack([first_real, first_imag, second_real, second_imag], axis=1)
    landed = lax.all_to_all(
        columns_to_sending(stacked, groups, slab, cols_own),
        "pix",
        split_axis=0,
        concat_axis=0,
        tiled=True,
    )
    row_layout = landed_to_rows(landed, groups, slab, cols_own)
    even_one, odd_one = transform_last(row_layout[:, 0], row_layout[:, 1], 1.0)
    even_two, odd_two = transform_last(row_layout[:, 2], row_layout[:, 3], 1.0)
    shear_one = jnp.stack([even_one, odd_one], axis=1).reshape(planes, slab, L)
    shear_two = jnp.stack([even_two, odd_two], axis=1).reshape(planes, slab, L)
    return (convergence, shear_one * scale, shear_two * scale)


INNER = 128
OUTER = L // INNER
HALF_BLOCKS = OUTER // 2


def block_columns():
    cols = np.zeros((HALF_BLOCKS, INNER), np.int64)
    for b in range(HALF_BLOCKS - 1):
        cols[b] = b + 1 + OUTER * np.arange(INNER)
    half = np.arange(INNER // 2)
    cols[-1] = np.concatenate([OUTER * half, HALF_BLOCKS + OUTER * half])
    return cols


def split_table(table):
    high = table.astype(jnp.bfloat16)
    low = (table - high.astype(np.float64)).astype(jnp.bfloat16)
    return high, low


def row_tables():
    n2 = np.arange(INNER)
    out = np.zeros((HALF_BLOCKS, 2 * INNER, 2 * INNER))
    cols = block_columns()
    for b in range(HALF_BLOCKS):
        angle = 2 * np.pi / L * ((n2[:, None] * cols[b][None, :]) % L)
        co, si = np.cos(angle), np.sin(angle)
        if b < HALF_BLOCKS - 1:
            out[b] = np.block([[co, -si], [si, co]])
        else:
            h = INNER // 2
            out[b, :INNER, :h] = co[:, :h]
            out[b, :INNER, INNER : INNER + h] = -si[:, :h]
            out[b, INNER:, h:INNER] = co[:, h:]
            out[b, INNER:, INNER + h :] = -si[:, h:]
    return split_table(out)


def column_tables():
    idx = np.arange(INNER)
    angle = 2 * np.pi / INNER * ((idx[:, None] * idx[None, :]) % INNER)
    co, si = np.cos(angle), np.sin(angle)
    return split_table(np.block([[co, si], [-si, co]]))


def twiddle_tables():
    angle = 2 * np.pi / L * (np.arange(OUTER)[:, None] * np.arange(INNER)[None, :])
    return np.cos(angle).astype(np.float32), (-np.sin(angle)).astype(np.float32)


def times_root(value, k, n, sign):
    re, im = value
    k = k % n
    if k == 0:
        return value
    if 4 * k == n:
        return (-im, re) if sign > 0 else (im, -re)
    angle = 2 * math.pi * k / n
    c, s = math.cos(angle), sign * math.sin(angle)
    if 8 * k == n or 8 * k == 3 * n:
        if c > 0:
            return ((re - im) * c, (re + im) * c) if sign > 0 else ((re + im) * c, (im - re) * c)
        c = -c
        return ((re + im) * -c, (re - im) * c) if sign > 0 else ((im - re) * c, (re + im) * -c)
    return (re * c - im * s, re * s + im * c)


def fft_list(values, sign):
    n = len(values)
    if n == 1:
        return values
    even = fft_list(values[0::2], sign)
    odd = fft_list(values[1::2], sign)
    odd = [times_root(v, k, n, sign) for k, v in enumerate(odd)]
    return [(a[0] + b[0], a[1] + b[1]) for a, b in zip(even, odd)] + [
        (a[0] - b[0], a[1] - b[1]) for a, b in zip(even, odd)
    ]


def split_value(value):
    high = value.astype(jnp.bfloat16)
    return high, (value - high.astype(jnp.float32)).astype(jnp.bfloat16)


def three_pass(left, right, dims):
    dot = lambda a, b: lax.dot_general(a, b, (dims, ((), ())), preferred_element_type=jnp.float32)
    return dot(left[0], right[0]) + (dot(left[0], right[1]) + dot(left[1], right[0]))


def deposit_kernel(slot_ref, cell_ref, mass_ref, *out_refs):
    planes, tiles, per_tile = cell_ref.shape
    groups, rows, _ = out_refs[0].shape
    cap = rows // TR
    row_id = lax.broadcasted_iota(jnp.int32, (TR, per_tile), 0)
    col_id = lax.broadcasted_iota(jnp.int32, (TC, per_tile), 0)
    for p in range(planes):
        out_ref = out_refs[p]
        out_ref[...] = jnp.zeros_like(out_ref)
        total = jnp.sum(jnp.sum(mass_ref[p].astype(jnp.float32), axis=0, keepdims=True), axis=1, keepdims=True)
        out_ref[:, cap * TR :, :] = jnp.broadcast_to(total[None], (groups, rows - cap * TR, TC))

        def batch(g, _):
            base = pl.multiple_of(g * 16, 16)
            cells = cell_ref[p, pl.ds(base, 16), :]
            weights = mass_ref[p, pl.ds(base, 16), :].astype(jnp.float32)
            for i in range(16):
                cell = cells[i : i + 1]
                weight = weights[i : i + 1]
                row_hot = jnp.where(row_id == cell // TC, weight, 0.0).astype(jnp.bfloat16)
                col_hot = jnp.where(col_id == cell % TC, 1.0, 0.0).astype(jnp.bfloat16)
                tile = lax.dot_general(
                    row_hot, col_hot, (((1,), (1,)), ((), ())), preferred_element_type=jnp.float32
                )
                slot = slot_ref[p, base + i]
                out_ref[slot // cap, pl.ds(pl.multiple_of((slot % cap) * TR, TR), TR), :] = tile
            return 0

        lax.fori_loop(0, tiles // 16, batch, 0)


def assemble_kernel(place_ref, in_ref, out_ref, held):
    groups, rows, _ = in_ref.shape
    cap = rows // TR
    tiles = out_ref.shape[0]
    held[...] = jnp.zeros_like(held)
    total = in_ref[0, cap * TR : cap * TR + 1, 0:1]
    for s in range(1, groups):
        total = total + in_ref[s, cap * TR : cap * TR + 1, 0:1]

    def source(s, _):
        for c in range(cap):
            at = place_ref[s * cap + c]
            held[at] = held[at] + in_ref[s, c * TR : (c + 1) * TR, :]
        return 0

    lax.fori_loop(0, groups, source, 0)
    factor = (L * L) / total
    out_ref[...] = held[0:tiles] * factor[None] - 1.0


def row_forward_kernel(mix_ref, near0, near1, far0, far1, high_ref, low_ref, conv_ref, out_ref, held):
    tile_rows = near0.shape[0] // OUTER

    def chunk(t, _):
        rows = pl.ds(pl.multiple_of(t * TR, TR), TR)
        packed = []
        for n in range(OUTER):
            at = t * OUTER + n
            fields = (near0[at], near1[at], far0[at], far1[at])
            pair = []
            for i in range(2):
                value = mix_ref[i, 0] * fields[0]
                for j in range(1, 4):
                    value = value + mix_ref[i, j] * fields[j]
                conv_ref[i, rows, n * INNER : (n + 1) * INNER] = value
                pair.append(value)
            packed.append(tuple(pair))
        z = fft_list(packed, -1)
        for k in range(1, HALF_BLOCKS):
            (ar, ai), (br, bi) = z[k], z[OUTER - k]
            held[k - 1, 0, rows, :INNER] = 0.5 * (ar + br)
            held[k - 1, 0, rows, INNER:] = 0.5 * (ai - bi)
            held[k - 1, 1, rows, :INNER] = 0.5 * (ai + bi)
            held[k - 1, 1, rows, INNER:] = 0.5 * (br - ar)
        for p in range(2):
            held[HALF_BLOCKS - 1, p, rows, :INNER] = z[0][p]
            held[HALF_BLOCKS - 1, p, rows, INNER:] = z[HALF_BLOCKS][p]
        return 0

    lax.fori_loop(0, tile_rows, chunk, 0)

    def block(b, _):
        slab = tile_rows * TR
        value = held[b].reshape(2 * slab, 2 * INNER)
        result = three_pass(split_value(value), (high_ref[b], low_ref[b]), ((1,), (0,)))
        for p in range(2):
            for half in range(2):
                out_ref[b, p, half] = result[
                    p * slab : (p + 1) * slab, half * INNER : (half + 1) * INNER
                ]
        return 0

    lax.fori_loop(0, HALF_BLOCKS, block, 0)


def column_inverse(f, col_ref, twr_ref, twi_ref, spectrum_of, back_high_ref, back_low_ref, out_ref, back):
    signed_v = col_ref[0:1]
    weight = col_ref[1:2]
    inner_id = lax.broadcasted_iota(jnp.int32, (INNER, INNER), 0)

    def middle(k, _):
        spectrum = spectrum_of(k)
        u = k + OUTER * inner_id
        signed_u = jnp.where(u >= L // 2, u - L, u).astype(jnp.float32)
        scale = jnp.where(u == L // 2, 0.0, weight)
        uu, vv = signed_u * signed_u, signed_v * signed_v
        over = scale / jnp.maximum(uu + vv, 1.0)
        kernel = (vv - uu) * over if f == 0 else 2.0 * signed_v * signed_u * over
        twice = jnp.concatenate([kernel, kernel], axis=0)
        result = three_pass(
            (back_high_ref[...], back_low_ref[...]), split_value(spectrum * twice), ((1,), (0,))
        )
        re, im = result[:INNER], result[INNER:]
        c, s = twr_ref[k], twi_ref[k]
        back[k, 0] = re * c + im * s
        back[k, 1] = im * c - re * s
        return 0

    lax.fori_loop(0, OUTER, middle, 0)

    def inverse(t, _):
        rows = pl.ds(pl.multiple_of(t * 8, 8), 8)
        x = fft_list([(back[k, 0, rows, :], back[k, 1, rows, :]) for k in range(OUTER)], 1)
        for n in range(OUTER):
            out_ref[n, 0, rows, :] = x[n][0]
            out_ref[n, 1, rows, :] = x[n][1]
        return 0

    lax.fori_loop(0, INNER // 8, inverse, 0)


def column_first_kernel(
    in_ref, col_ref, twr_ref, twi_ref, high_ref, low_ref, back_high_ref, back_low_ref, out_ref, spec_ref, held, back
):
    def forward(t, _):
        rows = pl.ds(pl.multiple_of(t * 8, 8), 8)
        z = fft_list([(in_ref[n, 0, rows, :], in_ref[n, 1, rows, :]) for n in range(OUTER)], -1)
        for k in range(OUTER):
            re, im = z[k]
            if k:
                c, s = twr_ref[k, rows, :], twi_ref[k, rows, :]
                re, im = re * c - im * s, re * s + im * c
            held[k, 0, rows, :] = re
            held[k, 1, rows, :] = im
        return 0

    lax.fori_loop(0, INNER // 8, forward, 0)

    def spectrum_of(k):
        value = held[k].reshape(2 * INNER, INNER)
        spectrum = three_pass((high_ref[...], low_ref[...]), split_value(value), ((1,), (0,)))
        spec_ref[k] = spectrum
        return spectrum

    column_inverse(0, col_ref, twr_ref, twi_ref, spectrum_of, back_high_ref, back_low_ref, out_ref, back)


def column_second_kernel(spec_ref, col_ref, twr_ref, twi_ref, back_high_ref, back_low_ref, out_ref, back):
    column_inverse(
        1, col_ref, twr_ref, twi_ref, lambda k: spec_ref[k], back_high_ref, back_low_ref, out_ref, back
    )


def row_inverse_kernel(in_ref, high_ref, low_ref, out_ref, held):
    slab = in_ref.shape[3]

    def block(b, _):
        value = jnp.concatenate(
            [jnp.concatenate([in_ref[b, p, 0], in_ref[b, p, 1]], axis=1) for p in range(2)], axis=0
        )
        held[b] = three_pass(split_value(value), (high_ref[b], low_ref[b]), ((1,), (1,))).reshape(
            2, slab, 2 * INNER
        )
        return 0

    lax.fori_loop(0, HALF_BLOCKS, block, 0)

    def chunk(t, _):
        rows = pl.ds(pl.multiple_of(t * 8, 8), 8)
        z = [None] * OUTER
        last = HALF_BLOCKS - 1
        z[0] = (held[last, 0, rows, :INNER], held[last, 1, rows, :INNER])
        z[HALF_BLOCKS] = (held[last, 0, rows, INNER:], held[last, 1, rows, INNER:])
        for k in range(1, HALF_BLOCKS):
            ar, ai = held[k - 1, 0, rows, :INNER], held[k - 1, 0, rows, INNER:]
            br, bi = held[k - 1, 1, rows, :INNER], held[k - 1, 1, rows, INNER:]
            z[k] = (ar - bi, ai + br)
            z[OUTER - k] = (ar + bi, br - ai)
        x = fft_list(z, 1)
        for n in range(OUTER):
            for p in range(2):
                out_ref[p, rows, n * INNER : (n + 1) * INNER] = x[n][p]
        return 0

    lax.fori_loop(0, slab // 8, chunk, 0)


def call(body, outs, scratch=(), smem=(0,), count=1, megabytes=48, flops=0):
    space = [
        pl.BlockSpec(memory_space=pltpu.SMEM if i in smem else pltpu.VMEM) for i in range(count)
    ]
    return pl.pallas_call(
        body,
        out_shape=outs,
        in_specs=space,
        out_specs=jax.tree.map(lambda _: pl.BlockSpec(memory_space=pltpu.VMEM), outs),
        scratch_shapes=list(scratch),
        compiler_params=pltpu.CompilerParams(vmem_limit_bytes=megabytes << 20),
        cost_estimate=pl.CostEstimate(flops=flops, bytes_accessed=4 << 20, transcendentals=0),
    )


def shape(*dims):
    return jax.ShapeDtypeStruct(dims, jnp.float32)


def local_fast(block_tile, cell_index, masses, plane_coef, plane_dist, source_inv):
    groups = lax.axis_size("pix")
    me = lax.axis_index("pix")
    mine_shell = lax.axis_index("shell")
    planes, local_tiles, per_tile = cell_index.shape
    slab = L // groups
    per_owner = slab // TR * (L // TC)
    cap = max(1, 2 * local_tiles // groups)

    pairs = [(0, 1)]
    other = lax.ppermute(jnp.concatenate([plane_coef, plane_dist]), "shell", pairs)
    other_coef = jnp.where(mine_shell > 0, other[:planes], 0.0)
    other_dist = other[planes:]

    table = block_tile.reshape(planes, groups, local_tiles)
    owner = table // per_owner
    earlier = jnp.arange(local_tiles)[:, None] < jnp.arange(local_tiles)[None, :]
    same_owner = owner[:, :, :, None] == owner[:, :, None, :]
    rank = jnp.sum(jnp.where(same_owner & earlier[None, None], 1, 0), axis=2)
    slot = owner * cap + rank
    my_slots = lax.dynamic_index_in_dim(slot, me, axis=1, keepdims=False)
    wanted = me * cap + jnp.arange(cap)
    here = slot[:, :, None, :] == wanted[None, None, :, None]
    local_index = table - me * per_owner
    place = jnp.sum(jnp.where(here, local_index[:, :, None, :] + 1, 0), axis=3)
    place = jnp.where(place > 0, place - 1, per_owner).reshape(planes, groups * cap)

    rows = cap * TR + 8
    outgoing = call(deposit_kernel, [shape(groups, rows, TC)] * planes, count=3, flops=1 << 29)(
        my_slots, cell_index, masses
    )
    near, far = [], []
    for p in range(planes):
        incoming = lax.all_to_all(outgoing[p], "pix", split_axis=0, concat_axis=0, tiled=True)
        contrast = call(
            assemble_kernel,
            shape(per_owner, TR, TC),
            [pltpu.VMEM((per_owner + 1, TR, TC), jnp.float32)],
            count=2,
            flops=1 << 22,
        )(place[p], incoming)
        near.append(contrast)
        far.append(lax.ppermute(contrast, "shell", pairs))

    own = plane_coef[None, :] * (1.0 - source_inv[:, None] * plane_dist[None, :])
    own = jnp.where(jnp.arange(planes)[None, :] <= jnp.arange(planes)[:, None], own, 0.0)
    before = other_coef[None, :] * (1.0 - source_inv[:, None] * other_dist[None, :])
    mix = jnp.concatenate([own, before], axis=1)

    row_high, row_low = row_tables()
    convergence, sending = call(
        row_forward_kernel,
        [shape(planes, slab, L), shape(HALF_BLOCKS, planes, 2, slab, INNER)],
        [pltpu.VMEM((HALF_BLOCKS, planes, slab, 2 * INNER), jnp.float32)],
        count=7,
        flops=1 << 30,
    )(mix, *near, *far, row_high, row_low)
    arrived = lax.all_to_all(
        sending.reshape(groups, 2, slab, INNER), "pix", split_axis=0, concat_axis=0, tiled=True
    )

    columns = jnp.asarray(block_columns().astype(np.float32))
    mine = lax.dynamic_index_in_dim(columns, me // planes, axis=0, keepdims=False)
    special = (me // planes == HALF_BLOCKS - 1) & (mine > 0)
    weight = jnp.where(special, 2.0, 1.0) / (L * L)
    signed = jnp.where(mine >= L // 2, mine - L, mine)
    col_info = jnp.stack([signed, weight])
    col_high, col_low = column_tables()
    tw_real, tw_imag = twiddle_tables()
    spread = lambda t: jnp.broadcast_to(jnp.asarray(t)[:, :, None], (OUTER, INNER, INNER))
    twiddles = (spread(tw_real), spread(tw_imag))
    backs = (col_high.T.copy(), col_low.T.copy())
    work = pltpu.VMEM((OUTER, 2, INNER, INNER), jnp.float32)
    leaving_one, spectrum = call(
        column_first_kernel,
        [shape(groups, 2, slab, INNER), shape(OUTER, 2 * INNER, INNER)],
        [work, work],
        smem=(),
        count=8,
        flops=1 << 31,
    )(arrived, col_info, *twiddles, col_high, col_low, *backs)
    landed_one = lax.all_to_all(leaving_one, "pix", split_axis=0, concat_axis=0, tiled=True)
    leaving_two = call(
        column_second_kernel,
        shape(groups, 2, slab, INNER),
        [work],
        smem=(),
        count=6,
        flops=1 << 31,
    )(spectrum, col_info, *twiddles, *backs)
    leaving_two, landed_one = lax.optimization_barrier((leaving_two, landed_one))
    landed_two = lax.all_to_all(leaving_two, "pix", split_axis=0, concat_axis=0, tiled=True)
    finish = lambda landed: call(
        row_inverse_kernel,
        shape(planes, slab, L),
        [pltpu.VMEM((HALF_BLOCKS, planes, slab, 2 * INNER), jnp.float32)],
        smem=(),
        count=3,
        flops=1 << 31,
    )(landed.reshape(HALF_BLOCKS, planes, 2, slab, INNER), row_high, row_low)
    shear_one = finish(landed_one)
    shear_two = finish(landed_two)
    return convergence, shear_one, shear_two


def solution(mesh):
    placed = (
        P("shell", None),
        P("shell", "pix", None),
        P("shell", "pix", None),
        P("shell"),
        P("shell"),
        P("shell"),
    )
    shells, groups = mesh.shape["shell"], mesh.shape["pix"]

    def body(block_tile, cell_index, *rest):
        fits = (
            shells == 2
            and cell_index.shape[0] == 2
            and groups == OUTER
            and cell_index.shape[1] % 16 == 0
        )
        return (local_fast if fits else local)(block_tile, cell_index, *rest)

    return jax.shard_map(
        body,
        mesh=mesh,
        in_specs=placed,
        out_specs=(P("shell", "pix", None), P("shell", "pix", None), P("shell", "pix", None)),
        check_vma=False,
    )
```

```python
from functools import partial
import math

import jax
import jax.numpy as jnp
from jax import lax
from jax.experimental import pallas as pl
from jax.experimental.pallas import tpu as pltpu
from jax.sharding import PartitionSpec as P
import numpy as np

L = 2048
TR = 16
TC = 128


HIGHEST = lax.Precision.HIGHEST


def entering(value, axis, join, neutral):
    count, mine = (lax.axis_size(axis), lax.axis_index(axis))
    pieces = jax.tree.map(lambda part: lax.all_gather(part, axis), value)
    running = jax.tree.map(
        lambda part, zero: jnp.full_like(part, 0) + jnp.asarray(zero, part.dtype), value, neutral
    )

    def lap(position, running):
        longer = join(running, jax.tree.map(lambda part: part[position], pieces))
        return jax.tree.map(lambda new, old: jnp.where(position < mine, new, old), longer, running)

    return lax.fori_loop(0, count - 1, lap, running)


def dft_table(left_size, right_size, period, sign_value):
    left_idx = jnp.arange(left_size)[:, None]
    right_idx = jnp.arange(right_size)[None, :]
    angle = 2.0 * math.pi / period * (left_idx * right_idx % period).astype(jnp.float32)
    return (jnp.cos(angle), sign_value * jnp.sin(angle))


def mix_outer(table, real_part, imag_part):
    cosine, sine_part = table
    contract = partial(jnp.einsum, "ab,...bc->...ac", precision=HIGHEST)
    return (
        contract(cosine, real_part) - contract(sine_part, imag_part),
        contract(sine_part, real_part) + contract(cosine, imag_part),
    )


def mix_inner(table, real_part, imag_part):
    cosine, sine_part = table
    product = partial(jnp.matmul, precision=HIGHEST)
    return (
        product(real_part, cosine) - product(imag_part, sine_part),
        product(real_part, sine_part) + product(imag_part, cosine),
    )


def twist(table, real_part, imag_part):
    cosine, sine_part = table
    return (real_part * cosine - imag_part * sine_part, real_part * sine_part + imag_part * cosine)


def transform_last(real_part, imag_part, sign_value):
    length = real_part.shape[-1]
    inner = math.gcd(length, 128)
    outer = length // inner
    leading = real_part.shape[:-1]
    real_part = real_part.reshape(leading + (outer, inner))
    imag_part = imag_part.reshape(leading + (outer, inner))
    outer_table = dft_table(outer, outer, outer, sign_value)
    inner_table = dft_table(inner, inner, inner, sign_value)
    twiddle = dft_table(outer, inner, length, sign_value)
    if sign_value < 0:
        real_part, imag_part = mix_outer(outer_table, real_part, imag_part)
        real_part, imag_part = twist(twiddle, real_part, imag_part)
        real_part, imag_part = mix_inner(inner_table, real_part, imag_part)
    else:
        real_part, imag_part = mix_inner(inner_table, real_part, imag_part)
        real_part, imag_part = twist(twiddle, real_part, imag_part)
        real_part, imag_part = mix_outer(outer_table, real_part, imag_part)
    return (real_part.reshape(leading + (length,)), imag_part.reshape(leading + (length,)))


def frequency_of(position, length):
    inner = math.gcd(length, 128)
    outer = length // inner
    frequency = position // inner + outer * (position % inner)
    signed = jnp.where(frequency >= length // 2, frequency - length, frequency).astype(jnp.float32)
    keep_mask = (frequency != length // 2).astype(jnp.float32)
    return (signed, keep_mask)


def add_pairs(earlier_pair, later_pair):
    return (earlier_pair[0] + later_pair[0], earlier_pair[1] + later_pair[1])


def deposit_group(item):
    cell_ids, weights = item
    tile_rows = cell_ids // TC
    tile_cols = cell_ids % TC
    row_hot = jnp.where(
        tile_rows[:, None, :] == jnp.arange(TR)[None, :, None],
        weights[:, None, :],
        jnp.zeros((), jnp.bfloat16),
    )
    col_hot = (tile_cols[:, :, None] == jnp.arange(TC)[None, None, :]).astype(jnp.bfloat16)
    return jnp.einsum("grk,gkc->grc", row_hot, col_hot, preferred_element_type=jnp.float32)


def rows_to_sending(packed, groups, slab, cols_own):
    count, fields = (packed.shape[0], packed.shape[1])
    return (
        packed.reshape(count, fields, slab, groups, cols_own)
        .transpose(3, 0, 1, 4, 2)
        .reshape(groups, count, fields, cols_own * slab)
    )


def arrived_to_columns(arrived, groups, slab, cols_own):
    count, fields = (arrived.shape[1], arrived.shape[2])
    return (
        arrived.reshape(groups, count, fields, cols_own, slab)
        .transpose(1, 2, 3, 0, 4)
        .reshape(count, fields, cols_own, groups * slab)
    )


def columns_to_sending(stacked, groups, slab, cols_own):
    count, fields = (stacked.shape[0], stacked.shape[1])
    return (
        stacked.reshape(count, fields, cols_own, groups, slab)
        .transpose(3, 0, 1, 2, 4)
        .reshape(groups, count, fields, cols_own * slab)
    )


def landed_to_rows(landed, groups, slab, cols_own):
    count, fields = (landed.shape[1], landed.shape[2])
    return (
        landed.reshape(groups, count, fields, cols_own, slab)
        .transpose(1, 2, 4, 0, 3)
        .reshape(count, fields, slab, groups * cols_own)
    )


def local(block_tile, cell_index, masses, plane_coef, plane_dist, source_inv):
    groups = lax.axis_size("pix")
    my_index = lax.axis_index("pix")
    planes, local_tiles, per_tile = cell_index.shape
    slab = L // groups
    per_owner = slab // TR * (L // TC)
    cap = max(1, 2 * local_tiles // groups)
    flat = TR * TC
    batch_tiles = 8
    deposited = lax.map(
        deposit_group,
        (cell_index.reshape(-1, batch_tiles, per_tile), masses.reshape(-1, batch_tiles, per_tile)),
    )
    tile_sums = deposited.reshape(planes, local_tiles, flat)
    table = block_tile.reshape(planes, groups, local_tiles)
    owner = table // per_owner
    earlier = jnp.arange(local_tiles)[:, None] < jnp.arange(local_tiles)[None, :]
    same_owner = owner[:, :, :, None] == owner[:, :, None, :]
    rank = jnp.sum(jnp.where(same_owner & earlier[None, None], 1, 0), axis=2)
    slot = owner * cap + rank
    my_slots = lax.dynamic_index_in_dim(slot, my_index, axis=1, keepdims=False)
    slot_grid = jnp.arange(groups)[:, None] * cap + jnp.arange(cap)[None, :]
    send_hot = (my_slots[:, None, None, :] == slot_grid[None, :, :, None]).astype(jnp.float32)
    outgoing = jnp.einsum("pnct,ptf->npcf", send_hot, tile_sums, precision=HIGHEST)
    incoming = lax.all_to_all(outgoing, "pix", split_axis=0, concat_axis=0, tiled=True)
    local_index = table - my_index * per_owner
    is_mine = owner == my_index
    tile_hot = (is_mine[..., None] & (local_index[..., None] == jnp.arange(per_owner))).astype(
        jnp.float32
    )
    slot_hot = (rank[..., None] == jnp.arange(cap)).astype(jnp.float32)
    placing = jnp.einsum("pstl,pstc->plsc", tile_hot, slot_hot, precision=HIGHEST)
    slab_tiles = jnp.einsum("plsc,spcf->plf", placing, incoming, precision=HIGHEST)
    density = (
        slab_tiles.reshape(planes, slab // TR, L // TC, TR, TC)
        .transpose(0, 1, 3, 2, 4)
        .reshape(planes, slab, L)
    )
    total = lax.psum(jnp.sum(density, axis=(1, 2)), "pix")
    contrast = density / (total / (L * L))[:, None, None] - 1.0
    near_local = jnp.cumsum(plane_coef[:, None, None] * contrast, axis=0)
    far_local = jnp.cumsum((plane_coef * plane_dist)[:, None, None] * contrast, axis=0)
    blank = jnp.zeros((slab, L), jnp.float32)
    near_before, far_before = entering(
        (near_local[-1], far_local[-1]), "shell", add_pairs, (blank, blank)
    )
    convergence = near_before + near_local - source_inv[:, None, None] * (far_before + far_local)
    cols_own = L // groups
    wave_x, keep_x = frequency_of(my_index * cols_own + jnp.arange(cols_own), L)
    wave_y, keep_y = frequency_of(jnp.arange(L), L)
    wave_x = wave_x[:, None]
    wave_y = wave_y[None, :]
    both_keep = keep_x[:, None] * keep_y[None, :]
    wave_power = jnp.maximum(wave_x * wave_x + wave_y * wave_y, 1.0)
    kernel_one = both_keep * (wave_x * wave_x - wave_y * wave_y) / wave_power
    kernel_two = both_keep * 2.0 * wave_x * wave_y / wave_power
    scale = 1.0 / (L * L)
    spec_real, spec_imag = transform_last(convergence[0::2], convergence[1::2], -1.0)
    sending = rows_to_sending(jnp.stack([spec_real, spec_imag], axis=1), groups, slab, cols_own)
    arrived = lax.all_to_all(sending, "pix", split_axis=0, concat_axis=0, tiled=True)
    columns = arrived_to_columns(arrived, groups, slab, cols_own)
    row_real, row_imag = transform_last(columns[:, 0], columns[:, 1], -1.0)
    first_real, first_imag = transform_last(row_real * kernel_one, row_imag * kernel_one, 1.0)
    second_real, second_imag = transform_last(row_real * kernel_two, row_imag * kernel_two, 1.0)
    stacked = jnp.stack([first_real, first_imag, second_real, second_imag], axis=1)
    landed = lax.all_to_all(
        columns_to_sending(stacked, groups, slab, cols_own),
        "pix",
        split_axis=0,
        concat_axis=0,
        tiled=True,
    )
    row_layout = landed_to_rows(landed, groups, slab, cols_own)
    even_one, odd_one = transform_last(row_layout[:, 0], row_layout[:, 1], 1.0)
    even_two, odd_two = transform_last(row_layout[:, 2], row_layout[:, 3], 1.0)
    shear_one = jnp.stack([even_one, odd_one], axis=1).reshape(planes, slab, L)
    shear_two = jnp.stack([even_two, odd_two], axis=1).reshape(planes, slab, L)
    return (convergence, shear_one * scale, shear_two * scale)


INNER = 128
OUTER = L // INNER
HALF_BLOCKS = OUTER // 2


def block_columns():
    cols = np.zeros((HALF_BLOCKS, INNER), np.int64)
    for b in range(HALF_BLOCKS - 1):
        cols[b] = b + 1 + OUTER * np.arange(INNER)
    half = np.arange(INNER // 2)
    cols[-1] = np.concatenate([OUTER * half, HALF_BLOCKS + OUTER * half])
    return cols


def split_table(table):
    high = table.astype(jnp.bfloat16)
    low = (table - high.astype(np.float64)).astype(jnp.bfloat16)
    return high, low


def row_tables():
    n2 = np.arange(INNER)
    out = np.zeros((HALF_BLOCKS, 2 * INNER, 2 * INNER))
    cols = block_columns()
    for b in range(HALF_BLOCKS):
        angle = 2 * np.pi / L * ((n2[:, None] * cols[b][None, :]) % L)
        co, si = np.cos(angle), np.sin(angle)
        if b < HALF_BLOCKS - 1:
            out[b] = np.block([[co, -si], [si, co]])
        else:
            h = INNER // 2
            out[b, :INNER, :h] = co[:, :h]
            out[b, :INNER, INNER : INNER + h] = -si[:, :h]
            out[b, INNER:, h:INNER] = co[:, h:]
            out[b, INNER:, INNER + h :] = -si[:, h:]
    return split_table(out)


def column_tables():
    idx = np.arange(INNER)
    angle = 2 * np.pi / INNER * ((idx[:, None] * idx[None, :]) % INNER)
    co, si = np.cos(angle), np.sin(angle)
    return split_table(np.block([[co, si], [-si, co]]))


def twiddle_tables():
    angle = 2 * np.pi / L * (np.arange(OUTER)[:, None] * np.arange(INNER)[None, :])
    return np.cos(angle).astype(np.float32), (-np.sin(angle)).astype(np.float32)


def times_root(value, k, n, sign):
    re, im = value
    k = k % n
    if k == 0:
        return value
    if 4 * k == n:
        return (-im, re) if sign > 0 else (im, -re)
    angle = 2 * math.pi * k / n
    c, s = math.cos(angle), sign * math.sin(angle)
    if 8 * k == n or 8 * k == 3 * n:
        if c > 0:
            return ((re - im) * c, (re + im) * c) if sign > 0 else ((re + im) * c, (im - re) * c)
        c = -c
        return ((re + im) * -c, (re - im) * c) if sign > 0 else ((im - re) * c, (re + im) * -c)
    return (re * c - im * s, re * s + im * c)


def fft_list(values, sign):
    n = len(values)
    if n == 1:
        return values
    even = fft_list(values[0::2], sign)
    odd = fft_list(values[1::2], sign)
    odd = [times_root(v, k, n, sign) for k, v in enumerate(odd)]
    return [(a[0] + b[0], a[1] + b[1]) for a, b in zip(even, odd)] + [
        (a[0] - b[0], a[1] - b[1]) for a, b in zip(even, odd)
    ]


def split_value(value):
    high = value.astype(jnp.bfloat16)
    return high, (value - high.astype(jnp.float32)).astype(jnp.bfloat16)


def three_pass(left, right, dims):
    dot = lambda a, b: lax.dot_general(a, b, (dims, ((), ())), preferred_element_type=jnp.float32)
    return dot(left[0], right[0]) + (dot(left[0], right[1]) + dot(left[1], right[0]))


def pack_kernel(slot_ref, list_ref, *out_refs):
    planes, tiles, size, _ = list_ref.shape
    groups, rows, _ = out_refs[0].shape
    cap = rows // size - 1
    for p in range(planes):
        out_ref = out_refs[p]
        out_ref[...] = jnp.zeros_like(out_ref)
        total = jnp.sum(list_ref[p, :, size // 2 :, :], axis=(0, 1))
        total = jnp.sum(total.reshape(1, TC), axis=1, keepdims=True)
        out_ref[:, cap * size :, :] = jnp.broadcast_to(total[None], (groups, size, TC))

        def tile(t, _):
            slot = slot_ref[p, t]
            rows_at = pl.ds(pl.multiple_of((slot % cap) * size, size), size)
            out_ref[slot // cap, rows_at, :] = list_ref[p, t]
            return 0

        lax.fori_loop(0, tiles, tile, 0)


def assemble_kernel(size, place_ref, in_ref, out_ref, held):
    groups, rows, _ = in_ref.shape
    cap = rows // size - 1
    tiles = out_ref.shape[0]
    half = size // 2
    held[...] = jnp.zeros_like(held)
    total = in_ref[0, cap * size : cap * size + 1, 0:1]
    for s in range(1, groups):
        total = total + in_ref[s, cap * size : cap * size + 1, 0:1]
    row_id = lax.broadcasted_iota(jnp.int32, (TR, TC), 0)
    col_id = lax.broadcasted_iota(jnp.int32, (TC, TC), 0)

    def source(s, _):
        for c in range(cap):
            at = place_ref[s * cap + c]
            entry = in_ref[s, c * size : (c + 1) * size, :]
            cells = entry[:half].astype(jnp.int32)
            row_hot, col_hot = [], []
            for i in range(half):
                cell = cells[i : i + 1]
                row_hot.append(jnp.where(row_id == cell // TC, entry[half + i : half + i + 1], 0.0))
                col_hot.append(jnp.where(col_id == cell % TC, 1.0, 0.0))
            held[at] = held[at] + lax.dot_general(
                jnp.concatenate(row_hot, axis=1).astype(jnp.bfloat16),
                jnp.concatenate(col_hot, axis=1).astype(jnp.bfloat16),
                (((1,), (1,)), ((), ())),
                preferred_element_type=jnp.float32,
            )
        return 0

    lax.fori_loop(0, groups, source, 0)
    factor = jnp.where(total > 0.0, (L * L) / total, 0.0)
    out_ref[...] = held[0:tiles] * factor[None] - 1.0


def row_forward_kernel(mix_ref, near0, near1, far0, far1, high_ref, low_ref, conv_ref, out_ref, held):
    tile_rows = near0.shape[0] // OUTER

    def chunk(t, _):
        rows = pl.ds(pl.multiple_of(t * TR, TR), TR)
        packed = []
        for n in range(OUTER):
            at = t * OUTER + n
            fields = (near0[at], near1[at], far0[at], far1[at])
            pair = []
            for i in range(2):
                value = mix_ref[i, 0] * fields[0]
                for j in range(1, 4):
                    value = value + mix_ref[i, j] * fields[j]
                conv_ref[i, rows, n * INNER : (n + 1) * INNER] = value
                pair.append(value)
            packed.append(tuple(pair))
        z = fft_list(packed, -1)
        for k in range(1, HALF_BLOCKS):
            (ar, ai), (br, bi) = z[k], z[OUTER - k]
            held[k - 1, 0, rows, :INNER] = 0.5 * (ar + br)
            held[k - 1, 0, rows, INNER:] = 0.5 * (ai - bi)
            held[k - 1, 1, rows, :INNER] = 0.5 * (ai + bi)
            held[k - 1, 1, rows, INNER:] = 0.5 * (br - ar)
        for p in range(2):
            held[HALF_BLOCKS - 1, p, rows, :INNER] = z[0][p]
            held[HALF_BLOCKS - 1, p, rows, INNER:] = z[HALF_BLOCKS][p]
        return 0

    lax.fori_loop(0, tile_rows, chunk, 0)

    def block(b, _):
        slab = tile_rows * TR
        value = held[b].reshape(2 * slab, 2 * INNER)
        result = three_pass(split_value(value), (high_ref[b], low_ref[b]), ((1,), (0,)))
        for p in range(2):
            for half in range(2):
                out_ref[b, p, half] = result[
                    p * slab : (p + 1) * slab, half * INNER : (half + 1) * INNER
                ]
        return 0

    lax.fori_loop(0, HALF_BLOCKS, block, 0)


def column_kernel(in_ref, col_ref, twr_ref, twi_ref, high_ref, low_ref, back_high_ref, back_low_ref, out_ref, held, *back):
    def twist_of(k, rows):
        return twr_ref[k, rows, :], twi_ref[k, rows, :]

    def forward(t, _):
        rows = pl.ds(pl.multiple_of(t * 8, 8), 8)
        z = fft_list([(in_ref[n, 0, rows, :], in_ref[n, 1, rows, :]) for n in range(OUTER)], -1)
        for k in range(OUTER):
            re, im = z[k]
            if k:
                c, s = twist_of(k, rows)
                re, im = re * c - im * s, re * s + im * c
            held[k, 0, rows, :] = re
            held[k, 1, rows, :] = im
        return 0

    lax.fori_loop(0, INNER // 8, forward, 0)
    signed_v = col_ref[0:1]
    weight = col_ref[1:2]
    inner_id = lax.broadcasted_iota(jnp.int32, (INNER, INNER), 0)

    def middle(k, _):
        value = held[k].reshape(2 * INNER, INNER)
        spectrum = three_pass((high_ref[...], low_ref[...]), split_value(value), ((1,), (0,)))
        u = k + OUTER * inner_id
        signed_u = jnp.where(u >= L // 2, u - L, u).astype(jnp.float32)
        scale = jnp.where(u == L // 2, 0.0, weight)
        uu, vv = signed_u * signed_u, signed_v * signed_v
        over = scale / jnp.maximum(uu + vv, 1.0)
        kernels = ((vv - uu) * over, 2.0 * signed_v * signed_u * over)
        for f in range(2):
            twice = jnp.concatenate([kernels[f], kernels[f]], axis=0)
            result = three_pass(
                (back_high_ref[...], back_low_ref[...]), split_value(spectrum * twice), ((1,), (0,))
            )
            re, im = result[:INNER], result[INNER:]
            c, s = twr_ref[k], twi_ref[k]
            back[f][k, 0] = re * c + im * s
            back[f][k, 1] = im * c - re * s
        return 0

    lax.fori_loop(0, OUTER, middle, 0)
    for f in range(2):

        def inverse(t, _):
            rows = pl.ds(pl.multiple_of(t * 8, 8), 8)
            x = fft_list([(back[f][k, 0, rows, :], back[f][k, 1, rows, :]) for k in range(OUTER)], 1)
            for n in range(OUTER):
                out_ref[n, f, 0, rows, :] = x[n][0]
                out_ref[n, f, 1, rows, :] = x[n][1]
            return 0

        lax.fori_loop(0, INNER // 8, inverse, 0)


def row_inverse_kernel(in_ref, high_ref, low_ref, one_ref, two_ref, held):
    slab = in_ref.shape[4]
    for f, out_ref in enumerate((one_ref, two_ref)):

        def block(b, _):
            value = jnp.concatenate(
                [jnp.concatenate([in_ref[b, p, f, 0], in_ref[b, p, f, 1]], axis=1) for p in range(2)], axis=0
            )
            held[b] = three_pass(split_value(value), (high_ref[b], low_ref[b]), ((1,), (1,))).reshape(
                2, slab, 2 * INNER
            )
            return 0

        lax.fori_loop(0, HALF_BLOCKS, block, 0)

        def chunk(t, _):
            rows = pl.ds(pl.multiple_of(t * 8, 8), 8)
            z = [None] * OUTER
            last = HALF_BLOCKS - 1
            z[0] = (held[last, 0, rows, :INNER], held[last, 1, rows, :INNER])
            z[HALF_BLOCKS] = (held[last, 0, rows, INNER:], held[last, 1, rows, INNER:])
            for k in range(1, HALF_BLOCKS):
                ar, ai = held[k - 1, 0, rows, :INNER], held[k - 1, 0, rows, INNER:]
                br, bi = held[k - 1, 1, rows, :INNER], held[k - 1, 1, rows, INNER:]
                z[k] = (ar - bi, ai + br)
                z[OUTER - k] = (ar + bi, br - ai)
            x = fft_list(z, 1)
            for n in range(OUTER):
                for p in range(2):
                    out_ref[p, rows, n * INNER : (n + 1) * INNER] = x[n][p]
            return 0

        lax.fori_loop(0, slab // 8, chunk, 0)


def call(body, outs, scratch=(), smem=(0,), count=1, megabytes=48, flops=0):
    space = [
        pl.BlockSpec(memory_space=pltpu.SMEM if i in smem else pltpu.VMEM) for i in range(count)
    ]
    return pl.pallas_call(
        body,
        out_shape=outs,
        in_specs=space,
        out_specs=jax.tree.map(lambda _: pl.BlockSpec(memory_space=pltpu.VMEM), outs),
        scratch_shapes=list(scratch),
        compiler_params=pltpu.CompilerParams(vmem_limit_bytes=megabytes << 20),
        cost_estimate=pl.CostEstimate(flops=flops, bytes_accessed=4 << 20, transcendentals=0),
    )


def shape(*dims):
    return jax.ShapeDtypeStruct(dims, jnp.float32)


def local_fast(block_tile, cell_index, masses, plane_coef, plane_dist, source_inv):
    groups = lax.axis_size("pix")
    me = lax.axis_index("pix")
    mine_shell = lax.axis_index("shell")
    planes, local_tiles, per_tile = cell_index.shape
    slab = L // groups
    per_owner = slab // TR * (L // TC)
    cap = max(1, 2 * local_tiles // groups)

    pairs = [(0, 1)]
    other = lax.ppermute(jnp.concatenate([plane_coef, plane_dist]), "shell", pairs)
    other_coef = jnp.where(mine_shell > 0, other[:planes], 0.0)
    other_dist = other[planes:]

    earlier = jnp.arange(local_tiles)[:, None] < jnp.arange(local_tiles)[None, :]
    wanted = me * cap + jnp.arange(cap)

    def routes(tiles):
        table = tiles.reshape(planes, groups, local_tiles)
        owner = table // per_owner
        same_owner = owner[:, :, :, None] == owner[:, :, None, :]
        rank = jnp.sum(jnp.where(same_owner & earlier[None, None], 1, 0), axis=2)
        slot = owner * cap + rank
        here = slot[:, :, None, :] == wanted[None, None, :, None]
        local_index = table - me * per_owner
        place = jnp.sum(jnp.where(here, local_index[:, :, None, :] + 1, 0), axis=3)
        place = jnp.where(place > 0, place - 1, per_owner).reshape(planes, groups * cap)
        return slot, place

    slot, place = routes(block_tile)
    _, other_place = routes(lax.ppermute(block_tile, "shell", pairs))
    my_slots = lax.dynamic_index_in_dim(slot, me, axis=1, keepdims=False)

    half = per_tile // TC
    as_lists = lambda part: part.astype(jnp.float32).reshape(planes, local_tiles, half, TC)
    lists = jnp.concatenate([as_lists(cell_index), as_lists(masses)], axis=2)
    outgoing = call(
        pack_kernel, [shape(groups, (cap + 1) * 2 * half, TC)] * planes, count=2, flops=1 << 20
    )(my_slots, lists)
    deposit = lambda where, entries: call(
        partial(assemble_kernel, 2 * half),
        shape(per_owner, TR, TC),
        [pltpu.VMEM((per_owner + 1, TR, TC), jnp.float32)],
        count=2,
        flops=1 << 31,
    )(where, entries)
    near, far = [], []
    for p in range(planes):
        incoming = lax.all_to_all(outgoing[p], "pix", split_axis=0, concat_axis=0, tiled=True)
        passed = lax.ppermute(incoming, "shell", pairs)
        near.append(deposit(place[p], incoming))
        far.append(deposit(other_place[p], passed))

    own = plane_coef[None, :] * (1.0 - source_inv[:, None] * plane_dist[None, :])
    own = jnp.where(jnp.arange(planes)[None, :] <= jnp.arange(planes)[:, None], own, 0.0)
    before = other_coef[None, :] * (1.0 - source_inv[:, None] * other_dist[None, :])
    mix = jnp.concatenate([own, before], axis=1)

    row_high, row_low = row_tables()
    convergence, sending = call(
        row_forward_kernel,
        [shape(planes, slab, L), shape(HALF_BLOCKS, planes, 2, slab, INNER)],
        [pltpu.VMEM((HALF_BLOCKS, planes, slab, 2 * INNER), jnp.float32)],
        count=7,
        flops=1 << 30,
    )(mix, *near, *far, row_high, row_low)
    arrived = lax.all_to_all(
        sending.reshape(groups, 2, slab, INNER), "pix", split_axis=0, concat_axis=0, tiled=True
    )

    columns = jnp.asarray(block_columns().astype(np.float32))
    mine = lax.dynamic_index_in_dim(columns, me // planes, axis=0, keepdims=False)
    special = (me // planes == HALF_BLOCKS - 1) & (mine > 0)
    weight = jnp.where(special, 2.0, 1.0) / (L * L)
    signed = jnp.where(mine >= L // 2, mine - L, mine)
    col_info = jnp.stack([signed, weight])
    col_high, col_low = column_tables()
    tw_real, tw_imag = twiddle_tables()
    spread = lambda t: jnp.broadcast_to(jnp.asarray(t)[:, :, None], (OUTER, INNER, INNER))
    leaving = call(
        column_kernel,
        shape(groups, 2, 2, slab, INNER),
        [pltpu.VMEM((OUTER, 2, INNER, INNER), jnp.float32)] * 3,
        smem=(),
        count=8,
        flops=1 << 31,
    )(arrived, col_info, spread(tw_real), spread(tw_imag), col_high, col_low, col_high.T.copy(), col_low.T.copy())
    landed = lax.all_to_all(leaving, "pix", split_axis=0, concat_axis=0, tiled=True)
    shear_one, shear_two = call(
        row_inverse_kernel,
        [shape(planes, slab, L)] * 2,
        [pltpu.VMEM((HALF_BLOCKS, planes, slab, 2 * INNER), jnp.float32)],
        smem=(),
        count=3,
        flops=1 << 31,
    )(landed.reshape(HALF_BLOCKS, planes, 2, 2, slab, INNER), row_high, row_low)
    return convergence, shear_one, shear_two


def solution(mesh):
    placed = (
        P("shell", None),
        P("shell", "pix", None),
        P("shell", "pix", None),
        P("shell"),
        P("shell"),
        P("shell"),
    )
    shells, groups = mesh.shape["shell"], mesh.shape["pix"]

    def body(block_tile, cell_index, *rest):
        fits = (
            shells == 2
            and cell_index.shape[0] == 2
            and groups == OUTER
            and cell_index.shape[2] % (4 * TC) == 0
        )
        return (local_fast if fits else local)(block_tile, cell_index, *rest)

    return jax.shard_map(
        body,
        mesh=mesh,
        in_specs=placed,
        out_specs=(P("shell", "pix", None), P("shell", "pix", None), P("shell", "pix", None)),
        check_vma=False,
    )
```
